32 devices in a mesh: rows: 8 (over y, x, core), planes: 4 (over z).
Axes of the slice: x: 2, y: 2, z: 4, core: 2. Of those that a mesh axis runs over, the one named last changes fastest.
Arguments:
- density: float32 [4, 4096, 4096], P('planes', 'rows'), may hold values from -6 to 6
- lens_weight: float32 [4], P('planes'), may hold values from 0.05 to 0.5
- spectrum_bin: int32 [4096, 4096], P(None, ('rows', 'planes')), may hold values from 0 to 63, as said below
Outputs:
- shear_real: float32 [4096, 4096], P(('rows', 'planes'))
- shear_imag: float32 [4096, 4096], P(('rows', 'planes'))
- spectrum: float32 [64], replicated
The draws below stay inside these ranges and needn't reach their ends.
Inputs may be any that keep to these rules, and one draw needn't show every extreme that they name: `spectrum_bin`: each Fourier pixel's band.
All inputs are finite; a program needn't handle non-finite values.
Results may differ from the reference program's by a relative error of at most 0.0003.
Values sent between devices are 32-bit elements; how exact they have to be, the bound alone decides.
A program may use at most 64 MiB of HBM per device.

```python
import math
import jax
import jax.numpy as jnp
from jax import lax

N = 4096
NBINS = 64
PLANES = 4


def draw_spectrum_bin(key, part):
    frequency = (jnp.arange(N, dtype=jnp.int32) + N // 2) % N - N // 2
    square_norm = frequency[:, None] ** 2 + frequency[None, :] ** 2
    radial = jnp.minimum(square_norm * NBINS // (N * N // 2), NBINS - 1)
    jitter = jax.random.randint(key, (N, N), -1, 2, dtype=jnp.int32)
    return jnp.clip(radial + jitter, 0, NBINS - 1).astype(jnp.int32)


def level_of(rng, shape, cuts, least, high):
    level = 1.0
    for axis_at, parts in cuts:
        draws = jax.random.uniform(jax.random.fold_in(jax.random.fold_in(rng, 6), axis_at), (parts,), jnp.float32, least / len(cuts), high / len(cuts))
        level = level * jnp.repeat(jnp.exp(draws), shape[axis_at] // parts).reshape((-1,) + (1,) * (len(shape) - 1 - axis_at))
    return level


def bell_draw(rng, dims, spread, limit, cuts=(), held_as=jnp.bfloat16):
    entries = spread * jax.random.normal(rng, dims, jnp.float32)
    if cuts:
        entries = entries * level_of(rng, dims, cuts, -0.22, 0.18)
    return jnp.clip(entries, -limit, limit).astype(held_as)


def setup_inputs(seed: int = 0) -> dict:
    keys = jax.random.split(jax.random.key(seed), 4)
    return {
        "density": bell_draw(keys[0], (PLANES, N, N), 1.0, 6.0, ((0, 4), (1, 8)), jnp.float32),
        "lens_weight": jnp.clip(jnp.exp(math.log(0.5) - 2.3025851 * jax.random.uniform(keys[1], (PLANES,), jnp.float32) ** level_of(keys[1], (PLANES,), ((0, 4),), -0.2, 0.2)), 0.05, 0.5),
        "spectrum_bin": draw_spectrum_bin(jax.random.fold_in(keys[3], 71), 0),
    }


def reference(density, lens_weight, spectrum_bin):
    def accumulate(plane_index, running):
        total_real, total_imag = running
        weighted_plane = density[plane_index] * lens_weight[plane_index]
        plane_hat = jnp.fft.fft2(weighted_plane)
        return (total_real + jnp.real(plane_hat), total_imag + jnp.imag(plane_hat))

    empty_sum = jnp.zeros((N, N), jnp.float32)
    total_real, total_imag = lax.fori_loop(0, PLANES, accumulate, (empty_sum, empty_sum))
    frequency = ((jnp.arange(N, dtype=jnp.int32) + N // 2) % N - N // 2).astype(jnp.float32)
    height = frequency[:, None]
    across = frequency[None, :]
    square_norm = height ** 2 + across ** 2
    anchor = square_norm == 0
    safe_norm = jnp.where(anchor, 1.0, square_norm)
    total_real = jnp.where(anchor, 0.0, total_real)
    total_imag = jnp.where(anchor, 0.0, total_imag)
    pixel_power = (total_real ** 2 + total_imag ** 2) * (NBINS / float(N) ** 4)
    spectrum = jax.ops.segment_sum(pixel_power.reshape(-1), spectrum_bin.reshape(-1), num_segments=NBINS)
    kernel_real = (across ** 2 - height ** 2) / safe_norm
    kernel_imag = 2.0 * across * height / safe_norm
    hat_real = kernel_real * total_real - kernel_imag * total_imag
    hat_imag = kernel_real * total_imag + kernel_imag * total_real
    shear_field = jnp.fft.ifft2(hat_real + 1j * hat_imag)
    return jnp.real(shear_field).astype(jnp.float32), jnp.imag(shear_field).astype(jnp.float32), spectrum
```

```python
import math

import jax
import jax.numpy as jnp
import numpy as np
from jax import lax
from jax.sharding import PartitionSpec as P

NBINS = 64
AXES = ("rows", "planes")


def phase(left, right, length, orient):
    index = np.arange(left)[:, None] * np.arange(right)[None, :] % length
    return np.exp(orient * 2j * math.pi * index / length)


def as_blocks(table):
    rows = np.stack([table.real, -table.imag], -1), np.stack([table.imag, table.real], -1)
    return np.stack(rows, 1).astype(np.float32)


def lane_table(table):
    top = np.concatenate([table.real, table.imag], 1)
    bottom = np.concatenate([-table.imag, table.real], 1)
    return np.concatenate([top, bottom], 0).astype(np.float32)


def product(pattern, left, right):
    return jnp.einsum(pattern, left, right, precision=lax.Precision.HIGH)


def turn(real, imag, table):
    cos, sin = table.real.astype(np.float32), table.imag.astype(np.float32)
    return real * cos - imag * sin, real * sin + imag * cos


def centred(indices, length):
    return ((indices + length // 2) % length - length // 2).astype(jnp.float32)


def plane_sum(density, lens_weight):
    count = lax.axis_size("planes")
    here = lax.axis_index("planes")
    block = density.shape[1] // count
    half = block // 2

    def own(owner, part):
        start = (owner % count) * block + part * half
        piece = lax.dynamic_slice_in_dim(density, start, half, axis=1)
        return jnp.sum(piece * lens_weight[:, None, None], axis=0)

    ways = ((0, 1), (1, -1))
    held = [own(here - way + count, part) for part, way in ways]
    for step in range(count - 1):
        moved = [
            lax.ppermute(held[part], "planes", [(i, (i + way) % count) for i in range(count)])
            for part, way in ways
        ]
        held = [
            moved[part] + own(here - way * (2 + step) + 2 * count, part) for part, way in ways
        ]
    return jnp.concatenate(held, axis=0)


def on_device(density, lens_weight, spectrum_bin):
    length = density.shape[-1]
    devices = lax.axis_size("rows") * lax.axis_size("planes")
    narrow = length // devices
    me = lax.axis_index("rows") * lax.axis_size("planes") + lax.axis_index("planes")

    share = plane_sum(density, lens_weight)
    field = share.T.reshape(narrow, devices, narrow)
    first = phase(narrow, narrow, narrow, -1)
    real = product("kn,nqy->kqy", first.real.astype(np.float32), field)
    imag = product("kn,nqy->kqy", first.imag.astype(np.float32), field)
    real, imag = turn(real, imag, phase(narrow, devices, length, -1)[:, :, None])
    forward = as_blocks(phase(devices, devices, devices, -1))
    spread = product("leq,kqy->leky", forward[..., 0], real) + product(
        "leq,kqy->leky", forward[..., 1], imag
    )
    held = lax.all_to_all(spread, AXES, split_axis=0, concat_axis=0, tiled=True)

    held = product("kesc,scxt->kext", forward, held)
    real, imag = turn(held[:, 0], held[:, 1], phase(devices, narrow, length, -1)[:, None, :])
    hat = product(
        "kxt,tm->kxm",
        jnp.concatenate([real, imag], -1),
        lane_table(phase(narrow, narrow, narrow, -1)),
    )
    hat_real, hat_imag = hat[..., :narrow], hat[..., narrow:]

    ky_index = (
        jnp.arange(devices, dtype=jnp.int32)[:, None, None]
        + devices * jnp.arange(narrow, dtype=jnp.int32)[None, None, :]
    )
    height = centred(ky_index, length)
    across = centred(me * narrow + jnp.arange(narrow, dtype=jnp.int32), length)[None, :, None]
    square_norm = height**2 + across**2
    anchor = square_norm == 0
    safe_norm = jnp.where(anchor, 1.0, square_norm)
    hat_real = jnp.where(anchor, 0.0, hat_real)
    hat_imag = jnp.where(anchor, 0.0, hat_imag)

    kernel_real = (across**2 - height**2) / safe_norm
    kernel_imag = 2.0 * across * height / safe_norm
    shear = jnp.concatenate(
        [
            kernel_real * hat_real - kernel_imag * hat_imag,
            kernel_real * hat_imag + kernel_imag * hat_real,
        ],
        -1,
    )
    back = product(
        "kxm,mt->kxt", shear, lane_table(phase(narrow, narrow, narrow, 1) / length)
    )
    real, imag = turn(
        back[..., :narrow], back[..., narrow:], phase(devices, narrow, length, 1)[:, None, :]
    )
    inverse = as_blocks(phase(devices, devices, devices, 1))
    back = product("sek,kxt->sext", inverse[..., 0], real) + product(
        "sek,kxt->sext", inverse[..., 1], imag
    )
    turned = lax.all_to_all(back, AXES, split_axis=0, concat_axis=0, tiled=True)

    pixel_power = (hat_real**2 + hat_imag**2) * (NBINS / float(length) ** 4)
    bins = spectrum_bin.reshape(narrow, devices, narrow).transpose(1, 2, 0)
    band_ids = jnp.arange(NBINS, dtype=jnp.int32)[:, None, None, None]
    partial_power = jnp.sum(jnp.where(bins == band_ids, pixel_power, 0.0), axis=(1, 2, 3))
    copies = jnp.broadcast_to(partial_power, (devices, 8, NBINS))
    gathered = lax.all_to_all(copies, AXES, split_axis=0, concat_axis=0, tiled=True)
    spectrum = jnp.sum(gathered[:, 0, :], axis=0)

    turned = product("aedc,dcqt->aeqt", inverse, turned)
    real, imag = turn(
        turned[:, 0], turned[:, 1], phase(devices, narrow, length, 1)[:, :, None]
    )
    last = phase(narrow, narrow, narrow, 1) / length
    cos, sin = last.real.astype(np.float32), last.imag.astype(np.float32)
    out_real = product("bq,aqt->bat", cos, real) - product("bq,aqt->bat", sin, imag)
    out_imag = product("bq,aqt->bat", sin, real) + product("bq,aqt->bat", cos, imag)
    shape = (length, narrow)
    return (out_real.reshape(shape).T, out_imag.reshape(shape).T, spectrum)


def solution(mesh):
    return jax.shard_map(
        on_device,
        mesh=mesh,
        in_specs=(P("planes", "rows", None), P("planes"), P(None, AXES)),
        out_specs=(P(AXES, None), P(AXES, None), P()),
        check_vma=False,
    )
```
